512 devices in a mesh: groups: 2 (over y), ctx: 32 (over z), head: 4 (over x), rep: 2 (over core).
Axes of the slice: x: 4, y: 2, z: 32, core: 2. Of those that a mesh axis runs over, the one named last changes fastest.
The devices are a block of a 4x16x32 slice.
Arguments:
- kv_cache: bfloat16 [4, 768, 128, 576], P(('groups', 'rep'), 'ctx'), parts along dimension 0, may hold values from -10 to 10
- queries: bfloat16 [4, 4, 128, 576], P(('groups', 'rep'), None, 'head'), parts along dimension 0, may hold values from -45 to 45
- new_latent: bfloat16 [4, 4, 576], P(('groups', 'rep')), parts along dimension 0, may hold values from -6 to 6
- page_counts: int32 [4, 4], P(('groups', 'rep')), parts along dimension 0, may hold values from 1 to 288, 576 in all within a row
- page_tails: int32 [4, 4], P(('groups', 'rep')), parts along dimension 0, may hold values from 1 to 128
- page_slots: int32 [4, 768], P(('groups', 'rep')), parts along dimension 0, may hold values from 0 to 767, each once within a row
Outputs:
- attended: bfloat16 [4, 4, 128, 512], P(('groups', 'rep'), None, 'head'), parts along dimension 0
The draws below stay inside these ranges and needn't reach their ends.
There are 2 independent parts, one for each index of `groups`. The reference program is written for one: setup_inputs(seed, part) draws one part's arguments, and reference() takes and returns one part's arrays. A program takes and returns all parts, laid end to end along the dimension named above; each array names one. Nothing has to cross between parts.
Inputs may be any that keep to these rules, and one draw needn't show every extreme that they name: `page_counts`: the 4 counts of a half sum to 576, and the largest is exactly 288. `page_slots`: each half's row holds every slot once; only its first 576 entries are pages in use.
All inputs are finite; a program needn't handle non-finite values.
Results may differ from the reference program's by a relative error of at most 0.0033.
Values sent between devices are 32-bit elements; how exact they have to be, the bound alone decides.
No kernel may reach another device: no remote copies, remote signals or barrier semaphores. Data moves between devices by JAX's collectives and lax.ppermute only.
A program may use at most 64 MiB of HBM per device.

```python
import math
import jax
import jax.numpy as jnp
import numpy as np
from jax import lax

HEADS = 128
LATENT = 512
PAGE = 128
BATCH = 4
KVW = 576
CTX_SLOTS = 768
TOTAL_PAGES = 576
MAXPAGES = 288
N_REP = 2


def draw_kv_cache(key, part):
    base = jnp.clip(jax.random.normal(jax.random.fold_in(key, 3), (N_REP, CTX_SLOTS, PAGE, KVW), jnp.float32), -6.0, 6.0)
    return base.astype(jnp.bfloat16)


def draw_queries(key, part):
    base = jnp.clip(jax.random.normal(jax.random.fold_in(key, 7), (N_REP, BATCH, HEADS, KVW), jnp.float32), -6.0, 6.0)
    return base.astype(jnp.bfloat16)


def plant(values, stream_key, low, largest):
    dims = values.shape
    place = [jax.random.randint(jax.random.fold_in(stream_key, axis), (), 0, dims[axis]) for axis in range(len(dims))]
    values = values.at[tuple(place)].set(low)
    longest = dims.index(max(dims))
    place[longest] = (place[longest] + 1) % dims[longest]
    return values.at[tuple(place)].set(largest)


def block_levels(own_key, shape, shards, low, high):
    def one(axis_at, shards_of):
        steps = jax.random.uniform(jax.random.fold_in(jax.random.fold_in(own_key, 6), axis_at), (shards_of,), jnp.float32, low / len(shards), high / len(shards))
        return jnp.repeat(jnp.exp(steps), shape[axis_at] // shards_of).reshape((-1,) + (1,) * (len(shape) - axis_at - 1))

    loudness = one(*shards[0])
    for cut in shards[1:]:
        loudness = loudness * one(*cut)
    return loudness


def length_profile(number_of, total, limit, skew):
    portions = [(1 << 20) // math.isqrt(rank ** skew) + 1 for rank in range(2, number_of + 1)]
    spare, given = total - limit - (number_of - 1), [1] * (number_of - 1)
    while spare > 0:
        movable = [i for i in range(number_of - 1) if given[i] < limit]
        whole, left = sum([portions[i] for i in movable]), spare
        for i in movable:
            more = min(limit - given[i], max(1, left * portions[i] // whole), spare)
            given[i] = given[i] + more
            spare = spare - more
    return np.array([limit] + given)


def ragged_sizes(key, count, total, reach, lean):
    if count == 2:
        one = jax.random.randint(key, (), max(1, total - reach), min(reach, total - 1) + 1)
        return jnp.stack([one, total - one])
    sizes = jnp.asarray(length_profile(count, total, reach, lean), jnp.int32)
    twos = (count - 1) // 2
    source_of, taker = sizes[1:1 + 2 * twos:2], sizes[2:2 + 2 * twos:2]
    margin = jnp.minimum(source_of - 1, reach - taker)
    moved = jax.random.randint(jax.random.fold_in(key, 1), (twos,), 0, 1 << 20) % (margin + 1)
    sizes = sizes.at[1:1 + 2 * twos:2].set(source_of - moved).at[2:2 + 2 * twos:2].set(taker + moved)
    return sizes[jax.random.permutation(jax.random.fold_in(key, 2), count)]


def gaussian(own_key, extent, width, limit, pieces=(), kind=jnp.bfloat16):
    level = block_levels(own_key, extent, pieces, -0.22, 0.18) if pieces else 1.0
    values = jax.random.normal(own_key, extent, jnp.float32) * width * level
    return jnp.minimum(jnp.maximum(values, -limit), limit).astype(kind)


def setup_inputs(seed: int = 0, part: int = 0) -> dict:
    key_list = jax.random.split(jax.random.key(seed), 7)
    part_keys = jax.random.split(jax.random.fold_in(key_list[6], part), 7)
    return {
        "kv_cache": draw_kv_cache(jax.random.fold_in(jax.random.fold_in(key_list[6], part), 71), part),
        "queries": draw_queries(jax.random.fold_in(jax.random.fold_in(key_list[6], part), 71), part),
        "new_latent": gaussian(part_keys[2], (N_REP, BATCH, KVW), 1.0, 6.0, ((0, 2),)),
        "page_counts": jax.vmap(lambda own: ragged_sizes(own, BATCH, TOTAL_PAGES, MAXPAGES, 2))(jax.random.split(part_keys[3], N_REP)).reshape((N_REP, BATCH)).astype(jnp.int32),
        "page_tails": plant(jax.random.randint(part_keys[4], (N_REP, BATCH), 1, PAGE + 1), jax.random.fold_in(part_keys[4], 1), 1, PAGE).astype(jnp.int32),
        "page_slots": jax.vmap(lambda own: jax.random.permutation(own, CTX_SLOTS))(jax.random.split(part_keys[5], N_REP)).reshape((N_REP, CTX_SLOTS)).astype(jnp.int32),
    }


score_scale = 192.0 ** -0.5
neg_large = -1.0e30


def page_partials(query_pages, cache_pages, token_valid):
    scores = jnp.einsum("phc,ptc->pht", query_pages.astype(jnp.float32), cache_pages.astype(jnp.float32)) * score_scale
    masked = jnp.where(token_valid[:, None, :], scores, neg_large)
    page_max = jnp.max(masked, axis=2)
    weights = jnp.where(token_valid[:, None, :], jnp.exp(masked - page_max[:, :, None]), 0.0).astype(jnp.bfloat16)
    page_sum = jnp.sum(weights.astype(jnp.float32), axis=2)
    page_acc = jnp.einsum("pht,ptc->phc", weights.astype(jnp.float32), cache_pages[:, :, :LATENT].astype(jnp.float32))
    return page_max, page_sum, page_acc


def reference(kv_cache, queries, new_latent, page_counts, page_tails, page_slots):
    halves = []
    for half in range(N_REP):
        counts = page_counts[half]
        ends = jnp.cumsum(counts).astype(jnp.int32)
        starts = (ends - counts).astype(jnp.int32)
        lengths = ((counts - 1) * PAGE + page_tails[half]).astype(jnp.int32)
        cache_half = kv_cache[half]
        slots_half = page_slots[half]

        def one_sequence(index):
            page_index = jnp.arange(MAXPAGES, dtype=jnp.int32)
            page_ok = page_index < jnp.take(counts, index)
            ranks = jnp.clip(jnp.take(starts, index) + page_index, 0, CTX_SLOTS - 1).astype(jnp.int32)
            slots = jnp.take(slots_half, ranks).astype(jnp.int32)
            cache_pages = jnp.take(cache_half, slots, axis=0)
            token_place = page_index[:, None] * PAGE + jnp.arange(PAGE, dtype=jnp.int32)[None, :]
            token_valid = page_ok[:, None] & (token_place < jnp.take(lengths, index))
            query_rows = queries[half][index]
            query_pages = jnp.broadcast_to(query_rows[None], (MAXPAGES,) + query_rows.shape)
            page_max, page_sum, page_acc = page_partials(query_pages, cache_pages, token_valid)
            own_row = new_latent[half][index].astype(jnp.float32)
            own_score = jnp.sum(query_rows.astype(jnp.float32) * own_row[None, :], axis=1) * score_scale
            top = jnp.maximum(jnp.max(page_max, axis=0), own_score)
            factor = jnp.exp(page_max - top[None, :])
            own_factor = jnp.exp(own_score - top)
            numer = jnp.sum(factor[:, :, None] * page_acc, axis=0) + own_factor[:, None] * own_row[None, :LATENT]
            denom = jnp.sum(factor * page_sum, axis=0) + own_factor
            return (numer / denom[:, None]).astype(jnp.bfloat16)

        halves.append(lax.map(one_sequence, jnp.arange(BATCH, dtype=jnp.int32)))
    return jnp.stack(halves)
```

```python
import jax
import jax.numpy as jnp
from jax import lax
from jax.experimental import pallas as pl
from jax.experimental.pallas import tpu as pltpu
from jax.sharding import PartitionSpec as P

LATENT = 512
CHUNK = 4

score_scale = 192.0 ** (-0.5)
neg_large = -1e30


def eye(n):
    return lax.broadcasted_iota(jnp.int32, (n, n), 0) == lax.broadcasted_iota(jnp.int32, (n, n), 1)


def as_row(col):
    n = col.shape[0]
    return jnp.sum(jnp.where(eye(n), jnp.broadcast_to(col, (n, n)), 0.0), axis=0, keepdims=True)


def as_col(row):
    n = row.shape[1]
    return jnp.sum(jnp.where(eye(n), jnp.broadcast_to(row, (n, n)), 0.0), axis=1, keepdims=True)


def fetch(kv_ref, kv_buf, sems):
    copies = []
    for i in range(kv_buf.shape[0] // CHUNK):
        part = pl.ds(i * CHUNK, CHUNK)
        copy = pltpu.make_async_copy(kv_ref.at[part], kv_buf.at[part], sems.at[i])
        copy.start()
        copies.append(copy)
    return copies


def score_kernel(place_ref, counts_ref, tails_ref, slots_ref, q_ref, new_ref, kv_ref, s_ref, m_ref, own_ref, kv_buf, bias_ref, sems):
    copies = fetch(kv_ref, kv_buf, sems)
    pages, _, width = kv_buf.shape
    rows = q_ref.shape[0]
    batch = new_ref.shape[0]
    heads = rows // batch
    slots = slots_ref[...]
    slot_ids = place_ref[0] * pages + lax.broadcasted_iota(jnp.int32, (pages, slots.shape[1]), 0)
    ranks_at = lax.broadcasted_iota(jnp.int32, (pages, slots.shape[1]), 1)
    rank = jnp.sum(jnp.where(slots == slot_ids, ranks_at, 0), axis=1, keepdims=True)
    token = lax.broadcasted_iota(jnp.int32, (pages, width), 1)
    start = jnp.int32(0)
    for b in range(batch):
        count = counts_ref[0, b]
        end = start + count
        length = (count - 1) * width + tails_ref[0, b]
        inside = (rank >= start) & (rank < end)
        limit = jnp.where(inside, length - (rank - start) * width, 0)
        bias_ref[b] = jnp.where(token < limit, 0.0, neg_large)
        start = end
    q = q_ref[...]
    own = []
    for b in range(batch):
        qb = q[b * heads : (b + 1) * heads].astype(jnp.float32)
        own.append(jnp.sum(qb * new_ref[b : b + 1, :].astype(jnp.float32), axis=1, keepdims=True) * score_scale)
    own = jnp.concatenate(own, axis=0)
    best = [jnp.full((heads, width), neg_large, jnp.float32) for _ in range(batch)]
    for i, copy in enumerate(copies):
        copy.wait()
        keys = jnp.concatenate([kv_buf[i * CHUNK + j] for j in range(CHUNK)], axis=1)
        scores = jnp.dot(q, keys, preferred_element_type=jnp.float32) * score_scale
        for j in range(CHUNK):
            p = i * CHUNK + j
            for b in range(batch):
                tile = scores[b * heads : (b + 1) * heads, j * width : (j + 1) * width] + bias_ref[b, p : p + 1, :]
                best[b] = jnp.maximum(best[b], tile)
                s_ref[b * heads : (b + 1) * heads, p * width : (p + 1) * width] = tile
    top = jnp.maximum(jnp.max(jnp.concatenate(best, axis=0), axis=1, keepdims=True), own)
    m_ref[...] = jnp.broadcast_to(as_row(top)[None], m_ref.shape)
    own_ref[...] = as_row(own)


def value_kernel(place_ref, s_ref, m_ref, own_ref, new_ref, kv_ref, acc_ref, sum_ref, kv_buf, sems):
    copies = fetch(kv_ref, kv_buf, sems)
    width = kv_buf.shape[2]
    rows = s_ref.shape[0]
    batch = new_ref.shape[0]
    heads = rows // batch
    top = as_col(m_ref[0])
    own_weight = jnp.where(place_ref[0] == 0, jnp.exp(as_col(own_ref[...]) - top), 0.0)
    total = jnp.zeros((rows, width), jnp.float32)
    acc = jnp.concatenate(
        [
            own_weight[b * heads : (b + 1) * heads] * new_ref[b : b + 1, :LATENT].astype(jnp.float32)
            for b in range(batch)
        ],
        axis=0,
    )
    for i, copy in enumerate(copies):
        copy.wait()
        span = CHUNK * width
        weights = jnp.exp(s_ref[:, i * span : (i + 1) * span] - top).astype(jnp.bfloat16)
        rounded = weights.astype(jnp.float32)
        for j in range(CHUNK):
            total = total + rounded[:, j * width : (j + 1) * width]
        values = jnp.concatenate([kv_buf[i * CHUNK + j, :LATENT, :] for j in range(CHUNK)], axis=1)
        acc = acc + lax.dot_general(weights, values, (((1,), (1,)), ((), ())), preferred_element_type=jnp.float32)
    acc_ref[...] = acc
    sum_ref[...] = as_row(jnp.sum(total, axis=1, keepdims=True) + own_weight)


def scale_kernel(acc_ref, sum_ref, m_ref, all_ref, *outs):
    everything = all_ref[...]
    top = jnp.max(everything, axis=0)
    factor = jnp.exp(m_ref[0] - top)
    first = lax.broadcasted_iota(jnp.int32, factor.shape, 1) == 0
    sums = sum_ref[...] * factor
    outs[-2][...] = jnp.where(first, 0.0, sums)
    outs[-1][...] = sums[:, :1]
    col = as_col(factor)
    at = 0
    for out in outs[:-2]:
        size = out.shape[0]
        out[...] = acc_ref[at : at + size, :] * col[at : at + size]
        at += size


def finish_kernel(*refs):
    parts, rest_ref, first_ref, out_ref = refs[:-3], refs[-3], refs[-2], refs[-1]
    first = lax.broadcasted_iota(jnp.int32, rest_ref.shape, 1) == 0
    sums = as_col(jnp.where(first, first_ref[...], rest_ref[...]))
    at = 0
    for part in parts:
        size = part.shape[0]
        out_ref[at : at + size, :] = (part[...] / sums[at : at + size]).astype(out_ref.dtype)
        at += size


def local(kv_cache, queries, new_latent, page_counts, page_tails, page_slots):
    _, pages, width, depth = kv_cache.shape
    _, batch, heads, _ = queries.shape
    rows = batch * heads
    members = lax.axis_size("ctx")
    kv = jnp.swapaxes(kv_cache[0], 1, 2)
    q = queries[0].reshape(rows, depth)
    new = new_latent[0]
    place = lax.axis_index("ctx").reshape(1)
    vmem = pl.BlockSpec(memory_space=pltpu.VMEM)
    smem = pl.BlockSpec(memory_space=pltpu.SMEM)
    hbm = pl.BlockSpec(memory_space=pl.ANY)
    f32 = jnp.float32
    kv_scratch = [pltpu.VMEM((pages, depth, width), kv.dtype)]
    sems = [pltpu.SemaphoreType.DMA((pages // CHUNK,))]
    scores, tops, own = pl.pallas_call(
        score_kernel,
        out_shape=(
            jax.ShapeDtypeStruct((rows, pages * width), f32),
            jax.ShapeDtypeStruct((members, 1, rows), f32),
            jax.ShapeDtypeStruct((1, rows), f32),
        ),
        in_specs=[smem, smem, smem, vmem, vmem, vmem, hbm],
        out_specs=(vmem, vmem, vmem),
        scratch_shapes=kv_scratch + [pltpu.VMEM((batch, pages, width), f32)] + sems,
        name="scores",
    )(place, page_counts, page_tails, page_slots, q, new, kv)
    all_tops = lax.all_to_all(tops, "ctx", 0, 0, tiled=True)
    acc, sums = pl.pallas_call(
        value_kernel,
        out_shape=(jax.ShapeDtypeStruct((rows, LATENT), f32), jax.ShapeDtypeStruct((1, rows), f32)),
        in_specs=[smem, vmem, vmem, vmem, vmem, hbm],
        out_specs=(vmem, vmem),
        scratch_shapes=kv_scratch + sems,
        name="values",
    )(place, scores, tops, own, new, kv)
    pieces = 8
    size = rows // pieces
    shapes = [jax.ShapeDtypeStruct((size, LATENT), f32)] * pieces
    shapes += [jax.ShapeDtypeStruct((1, rows), f32), jax.ShapeDtypeStruct((1, 1), f32)]
    scaled = pl.pallas_call(
        scale_kernel, out_shape=tuple(shapes), in_specs=[vmem] * 4, out_specs=(vmem,) * len(shapes), name="scale"
    )(acc, sums, tops, all_tops)
    summed = lax.psum(tuple(scaled), "ctx")
    out = pl.pallas_call(
        finish_kernel,
        out_shape=jax.ShapeDtypeStruct((rows, LATENT), jnp.bfloat16),
        in_specs=[vmem] * len(shapes),
        out_specs=vmem,
        name="finish",
    )(*summed)
    return out.reshape(1, batch, heads, LATENT)


def solution(mesh):
    in_specs = (
        P(("groups", "rep"), "ctx", None, None),
        P(("groups", "rep"), None, "head", None),
        P(("groups", "rep"), None, None),
        P(("groups", "rep"), None),
        P(("groups", "rep"), None),
        P(("groups", "rep"), None),
    )
    out_specs = P(("groups", "rep"), None, "head", None)
    return jax.shard_map(local, mesh=mesh, in_specs=in_specs, out_specs=out_specs, check_vma=False)
```

```python
import jax
import jax.numpy as jnp
from jax import lax
from jax.experimental import pallas as pl
from jax.experimental.pallas import tpu as pltpu
from jax.sharding import Mesh, PartitionSpec as P

LATENT = 512
LANES = 128
CHUNK = 4
BLOCK = 4


score_scale = 192.0 ** (-0.5)
neg_large = -1e30
CTX = ("ctx_block", "ctx_place")


def diagonal(rows):
    shape = (rows, LANES)
    return lax.broadcasted_iota(jnp.int32, shape, 0) == lax.broadcasted_iota(jnp.int32, shape, 1)


def as_row(col):
    return jnp.sum(jnp.where(diagonal(col.shape[0]), col, 0.0), axis=0, keepdims=True)


def as_col(row, rows):
    return jnp.sum(jnp.where(diagonal(rows), row, 0.0), axis=1, keepdims=True)


def tail_tile(top, total):
    at = lax.broadcasted_iota(jnp.int32, (8, LANES), 0)
    return jnp.where(at == 0, as_row(top), jnp.where(at == 1, as_row(total), 0.0))


def packed_rows(rows):
    return rows * (LATENT // LANES) + 8


def fetch(kv_ref, kv_buf, sems):
    copies = []
    for i in range(kv_buf.shape[0] // CHUNK):
        part = pl.ds(i * CHUNK, CHUNK)
        copy = pltpu.make_async_copy(kv_ref.at[part], kv_buf.at[part], sems.at[i])
        copy.start()
        copies.append(copy)
    return copies


def partial_kernel(place_ref, counts_ref, tails_ref, slots_ref, q_ref, new_ref, kv_ref, out_ref, kv_buf, s_buf, bias_ref, sems):
    copies = fetch(kv_ref, kv_buf, sems)
    pages, _, width = kv_buf.shape
    rows = q_ref.shape[0]
    batch = new_ref.shape[0]
    heads = rows // batch
    slots = slots_ref[...]
    slot_ids = place_ref[0] * pages + lax.broadcasted_iota(jnp.int32, (pages, slots.shape[1]), 0)
    ranks_at = lax.broadcasted_iota(jnp.int32, (pages, slots.shape[1]), 1)
    rank = jnp.sum(jnp.where(slots == slot_ids, ranks_at, 0), axis=1, keepdims=True)
    token = lax.broadcasted_iota(jnp.int32, (pages, width), 1)
    start = jnp.int32(0)
    for b in range(batch):
        count = counts_ref[0, b]
        end = start + count
        length = (count - 1) * width + tails_ref[0, b]
        inside = (rank >= start) & (rank < end)
        limit = jnp.where(inside, length - (rank - start) * width, 0)
        bias_ref[b] = jnp.where(token < limit, 0.0, neg_large)
        start = end
    q = q_ref[...]
    own = []
    for b in range(batch):
        qb = q[b * heads : (b + 1) * heads].astype(jnp.float32)
        own.append(jnp.sum(qb * new_ref[b : b + 1, :].astype(jnp.float32), axis=1, keepdims=True) * score_scale)
    own = jnp.concatenate(own, axis=0)
    best = [jnp.full((heads, width), neg_large, jnp.float32) for _ in range(batch)]
    for i, copy in enumerate(copies):
        copy.wait()
        keys = jnp.concatenate([kv_buf[i * CHUNK + j] for j in range(CHUNK)], axis=1)
        scores = jnp.dot(q, keys, preferred_element_type=jnp.float32) * score_scale
        for j in range(CHUNK):
            p = i * CHUNK + j
            for b in range(batch):
                tile = scores[b * heads : (b + 1) * heads, j * width : (j + 1) * width] + bias_ref[b, p : p + 1, :]
                best[b] = jnp.maximum(best[b], tile)
                s_buf[b * heads : (b + 1) * heads, p * width : (p + 1) * width] = tile
    top = jnp.maximum(jnp.max(jnp.concatenate(best, axis=0), axis=1, keepdims=True), own)
    own_weight = jnp.where(place_ref[0] == 0, jnp.exp(own - top), 0.0)
    total = jnp.zeros((rows, width), jnp.float32)
    acc = jnp.concatenate(
        [
            own_weight[b * heads : (b + 1) * heads] * new_ref[b : b + 1, :LATENT].astype(jnp.float32)
            for b in range(batch)
        ],
        axis=0,
    )
    for i in range(len(copies)):
        span = CHUNK * width
        weights = jnp.exp(s_buf[:, i * span : (i + 1) * span] - top).astype(jnp.bfloat16)
        rounded = weights.astype(jnp.float32)
        for j in range(CHUNK):
            total = total + rounded[:, j * width : (j + 1) * width]
        values = jnp.concatenate([kv_buf[i * CHUNK + j, :LATENT, :] for j in range(CHUNK)], axis=1)
        acc = acc + lax.dot_general(weights, values, (((1,), (1,)), ((), ())), preferred_element_type=jnp.float32)
    sums = jnp.sum(total, axis=1, keepdims=True) + own_weight
    members = out_ref.shape[0]
    size = rows // members
    for j in range(members):
        mine = slice(j * size, (j + 1) * size)
        for k in range(LATENT // LANES):
            out_ref[j, k * size : (k + 1) * size, :] = acc[mine, k * LANES : (k + 1) * LANES]
        out_ref[j, out_ref.shape[1] - 8 :, :] = tail_tile(top[mine], sums[mine])


def merged(pieces, rows):
    tops = [as_col(piece[piece.shape[0] - 8 : piece.shape[0] - 7, :], rows) for piece in pieces]
    sums = [as_col(piece[piece.shape[0] - 7 : piece.shape[0] - 6, :], rows) for piece in pieces]
    top = tops[0]
    for other in tops[1:]:
        top = jnp.maximum(top, other)
    factors = [jnp.exp(t - top) for t in tops]
    total = sum(f * s for f, s in zip(factors, sums))
    acc = []
    for k in range(LATENT // LANES):
        acc.append(sum(f * piece[k * rows : (k + 1) * rows, :] for f, piece in zip(factors, pieces)))
    return top, total, acc


def merge_kernel(in_ref, out_ref):
    members = in_ref.shape[0]
    rows = (out_ref.shape[0] - 8) // (LATENT // LANES)
    top, total, acc = merged([in_ref.at[i] for i in range(members)], rows)
    for k, part in enumerate(acc):
        out_ref[k * rows : (k + 1) * rows, :] = part
    out_ref[out_ref.shape[0] - 8 :, :] = tail_tile(top, total)


def close_kernel(*refs):
    pieces, out_ref = refs[:-1], refs[-1]
    rows = out_ref.shape[0] // (LATENT // LANES)
    _, total, acc = merged(pieces, rows)
    for k, part in enumerate(acc):
        out_ref[k * rows : (k + 1) * rows, :] = part / total


def choose_kernel(block_ref, own_ref, *refs):
    others, out_ref = refs[:-1], refs[-1]
    arrived = others[0][...]
    for other in others[1:]:
        arrived = arrived + other[...]
    out_ref[...] = jnp.where(block_ref[0] == 0, own_ref[...], arrived)


def unpack_kernel(in_ref, out_ref):
    members, packed, _ = in_ref.shape
    rows = packed // (LATENT // LANES)
    for j in range(members):
        for k in range(LATENT // LANES):
            tile = in_ref[j, k * rows : (k + 1) * rows, :]
            out_ref[j * rows : (j + 1) * rows, k * LANES : (k + 1) * LANES] = tile.astype(out_ref.dtype)


def local(kv_cache, queries, new_latent, page_counts, page_tails, page_slots):
    _, pages, width, depth = kv_cache.shape
    _, batch, heads, _ = queries.shape
    rows = batch * heads
    blocks, members = lax.axis_size("ctx_block"), lax.axis_size("ctx_place")
    kv = jnp.swapaxes(kv_cache[0], 1, 2)
    q = queries[0].reshape(rows, depth)
    new = new_latent[0]
    block = lax.axis_index("ctx_block").reshape(1)
    place = lax.axis_index(CTX).reshape(1)
    vmem = pl.BlockSpec(memory_space=pltpu.VMEM)
    smem = pl.BlockSpec(memory_space=pltpu.SMEM)
    hbm = pl.BlockSpec(memory_space=pl.ANY)
    f32 = jnp.float32
    size = rows // members
    packed = packed_rows(size)
    partials = pl.pallas_call(
        partial_kernel,
        out_shape=jax.ShapeDtypeStruct((members, packed, LANES), f32),
        in_specs=[smem, smem, smem, vmem, vmem, vmem, hbm],
        out_specs=vmem,
        scratch_shapes=[
            pltpu.VMEM((pages, depth, width), kv.dtype),
            pltpu.VMEM((rows, pages * width), f32),
            pltpu.VMEM((batch, pages, width), f32),
            pltpu.SemaphoreType.DMA((pages // CHUNK,)),
        ],
        name="partials",
    )(place, page_counts, page_tails, page_slots, q, new, kv)
    partials = lax.all_to_all(partials, "ctx_place", 0, 0, tiled=True)
    mine = pl.pallas_call(
        merge_kernel,
        out_shape=jax.ShapeDtypeStruct((packed, LANES), f32),
        in_specs=[vmem],
        out_specs=vmem,
        name="merge",
    )(partials)
    gathered = [
        lax.ppermute(mine, CTX, [(b * members + j, j) for j in range(members)]) for b in range(1, blocks)
    ]
    share = pl.pallas_call(
        close_kernel,
        out_shape=jax.ShapeDtypeStruct((packed - 8, LANES), f32),
        in_specs=[vmem] * blocks,
        out_specs=vmem,
        name="close",
    )(mine, *gathered)
    spread = [
        lax.ppermute(share, CTX, [(j, b * members + j) for j in range(members)]) for b in range(1, blocks)
    ]
    share = pl.pallas_call(
        choose_kernel,
        out_shape=jax.ShapeDtypeStruct(share.shape, f32),
        in_specs=[smem] + [vmem] * blocks,
        out_specs=vmem,
        name="choose",
    )(block, share, *spread)
    shares = lax.all_gather(share, "ctx_place", axis=0)
    out = pl.pallas_call(
        unpack_kernel,
        out_shape=jax.ShapeDtypeStruct((rows, LATENT), jnp.bfloat16),
        in_specs=[vmem],
        out_specs=vmem,
        name="unpack",
    )(shares)
    return out.reshape(1, batch, heads, LATENT)


def solution(mesh):
    groups, ctx, head, rep = (mesh.shape[a] for a in ("groups", "ctx", "head", "rep"))
    devices = mesh.devices.reshape(groups, ctx // BLOCK, BLOCK, head, rep)
    split = Mesh(devices, ("groups", *CTX, "head", "rep"))
    in_specs = (
        P(("groups", "rep"), CTX, None, None),
        P(("groups", "rep"), None, "head", None),
        P(("groups", "rep"), None, None),
        P(("groups", "rep"), None),
        P(("groups", "rep"), None),
        P(("groups", "rep"), None),
    )
    out_specs = P(("groups", "rep"), None, "head", None)
    return jax.shard_map(local, mesh=split, in_specs=in_specs, out_specs=out_specs, check_vma=False)
```

```python
import jax
import jax.numpy as jnp
from jax import lax
from jax.experimental import pallas as pl
from jax.experimental.pallas import tpu as pltpu
from jax.sharding import Mesh, PartitionSpec as P

LATENT = 512
LANES = 128
CHUNK = 4
BLOCK = 4


score_scale = 192.0 ** (-0.5)
neg_large = -1e30
CTX = ("ctx_block", "ctx_place")


def diagonal(rows):
    shape = (rows, LANES)
    return lax.broadcasted_iota(jnp.int32, shape, 0) == lax.broadcasted_iota(jnp.int32, shape, 1)


def as_row(col):
    return jnp.sum(jnp.where(diagonal(col.shape[0]), col, 0.0), axis=0, keepdims=True)


def as_col(row, rows):
    return jnp.sum(jnp.where(diagonal(rows), row, 0.0), axis=1, keepdims=True)


def tail_tile(top, total):
    at = lax.broadcasted_iota(jnp.int32, (8, LANES), 0)
    return jnp.where(at == 0, as_row(top), jnp.where(at == 1, as_row(total), 0.0))


def packed_rows(rows):
    return rows * (LATENT // LANES) + 8


def fetch(kv_ref, kv_buf, sems):
    copies = []
    for i in range(kv_buf.shape[0] // CHUNK):
        part = pl.ds(i * CHUNK, CHUNK)
        copy = pltpu.make_async_copy(kv_ref.at[part], kv_buf.at[part], sems.at[i])
        copy.start()
        copies.append(copy)
    return copies


def partial_kernel(place_ref, counts_ref, tails_ref, slots_ref, q_ref, new_ref, kv_ref, out_ref, kv_buf, s_buf, bias_ref, sems):
    copies = fetch(kv_ref, kv_buf, sems)
    pages, _, width = kv_buf.shape
    rows = q_ref.shape[0]
    batch = new_ref.shape[0]
    heads = rows // batch
    slots = slots_ref[...]
    slot_ids = place_ref[0] * pages + lax.broadcasted_iota(jnp.int32, (pages, slots.shape[1]), 0)
    ranks_at = lax.broadcasted_iota(jnp.int32, (pages, slots.shape[1]), 1)
    rank = jnp.sum(jnp.where(slots == slot_ids, ranks_at, 0), axis=1, keepdims=True)
    token = lax.broadcasted_iota(jnp.int32, (pages, width), 1)
    start = jnp.int32(0)
    for b in range(batch):
        count = counts_ref[0, b]
        end = start + count
        length = (count - 1) * width + tails_ref[0, b]
        inside = (rank >= start) & (rank < end)
        limit = jnp.where(inside, length - (rank - start) * width, 0)
        bias_ref[b] = jnp.where(token < limit, 0.0, neg_large)
        start = end
    q = q_ref[...]
    own = []
    for b in range(batch):
        qb = q[b * heads : (b + 1) * heads].astype(jnp.float32)
        own.append(jnp.sum(qb * new_ref[b : b + 1, :].astype(jnp.float32), axis=1, keepdims=True) * score_scale)
    own = jnp.concatenate(own, axis=0)
    best = [jnp.full((heads, width), neg_large, jnp.float32) for _ in range(batch)]
    for i, copy in enumerate(copies):
        copy.wait()
        keys = jnp.concatenate([kv_buf[i * CHUNK + j] for j in range(CHUNK)], axis=1)
        scores = jnp.dot(q, keys, preferred_element_type=jnp.float32) * score_scale
        for j in range(CHUNK):
            p = i * CHUNK + j
            for b in range(batch):
                tile = scores[b * heads : (b + 1) * heads, j * width : (j + 1) * width] + bias_ref[b, p : p + 1, :]
                best[b] = jnp.maximum(best[b], tile)
                s_buf[b * heads : (b + 1) * heads, p * width : (p + 1) * width] = tile
    top = jnp.maximum(jnp.max(jnp.concatenate(best, axis=0), axis=1, keepdims=True), own)
    own_weight = jnp.where(place_ref[0] == 0, jnp.exp(own - top), 0.0)
    total = jnp.zeros((rows, width), jnp.float32)
    acc = jnp.concatenate(
        [
            own_weight[b * heads : (b + 1) * heads] * new_ref[b : b + 1, :LATENT].astype(jnp.float32)
            for b in range(batch)
        ],
        axis=0,
    )
    for i in range(len(copies)):
        span = CHUNK * width
        weights = jnp.exp(s_buf[:, i * span : (i + 1) * span] - top).astype(jnp.bfloat16)
        rounded = weights.astype(jnp.float32)
        for j in range(CHUNK):
            total = total + rounded[:, j * width : (j + 1) * width]
        values = jnp.concatenate([kv_buf[i * CHUNK + j, :LATENT, :] for j in range(CHUNK)], axis=1)
        acc = acc + lax.dot_general(weights, values, (((1,), (1,)), ((), ())), preferred_element_type=jnp.float32)
    sums = jnp.sum(total, axis=1, keepdims=True) + own_weight
    members = out_ref.shape[0]
    size = rows // members
    for j in range(members):
        mine = slice(j * size, (j + 1) * size)
        for k in range(LATENT // LANES):
            out_ref[j, k * size : (k + 1) * size, :] = acc[mine, k * LANES : (k + 1) * LANES]
        out_ref[j, out_ref.shape[1] - 8 :, :] = tail_tile(top[mine], sums[mine])


def merged(pieces, rows):
    tops = [as_col(piece[piece.shape[0] - 8 : piece.shape[0] - 7, :], rows) for piece in pieces]
    sums = [as_col(piece[piece.shape[0] - 7 : piece.shape[0] - 6, :], rows) for piece in pieces]
    top = tops[0]
    for other in tops[1:]:
        top = jnp.maximum(top, other)
    factors = [jnp.exp(t - top) for t in tops]
    total = sum(f * s for f, s in zip(factors, sums))
    acc = []
    for k in range(LATENT // LANES):
        acc.append(sum(f * piece[k * rows : (k + 1) * rows, :] for f, piece in zip(factors, pieces)))
    return top, total, acc


def merge_kernel(in_ref, out_ref):
    members = in_ref.shape[0]
    rows = (out_ref.shape[0] - 8) // (LATENT // LANES)
    top, total, acc = merged([in_ref.at[i] for i in range(members)], rows)
    for k, part in enumerate(acc):
        out_ref[k * rows : (k + 1) * rows, :] = part
    out_ref[out_ref.shape[0] - 8 :, :] = tail_tile(top, total)


def close_kernel(*refs):
    pieces, out_ref = refs[:-1], refs[-1]
    rows = out_ref.shape[0] // (LATENT // LANES)
    _, total, acc = merged(pieces, rows)
    for k, part in enumerate(acc):
        out_ref[k * rows : (k + 1) * rows, :] = part / total


def choose_kernel(block_ref, own_ref, *refs):
    others, out_ref = refs[:-1], refs[-1]
    arrived = others[0][...]
    for other in others[1:]:
        arrived = arrived + other[...]
    blocks = lax.axis_size(CTX[0])
    closes = (block_ref[0] == 0) | (block_ref[0] == blocks // 2)
    share = jnp.where(closes, own_ref[...], arrived)
    for j in range(out_ref.shape[0]):
        out_ref[j] = share


def unpack_kernel(in_ref, out_ref):
    members, packed, _ = in_ref.shape
    rows = packed // (LATENT // LANES)
    for j in range(members):
        for k in range(LATENT // LANES):
            tile = in_ref[j, k * rows : (k + 1) * rows, :]
            out_ref[j * rows : (j + 1) * rows, k * LANES : (k + 1) * LANES] = tile.astype(out_ref.dtype)


def near(x):
    return pltpu.with_memory_space_constraint(x, pltpu.VMEM)


def inward(blocks):
    half = blocks // 2
    first = list(range(blocks - 1, 0, -1))
    second = [b for b in range(blocks - 1, -1, -1) if b != half]
    for i in range(0, half - 1, 2):
        second[i], second[i + 1] = second[i + 1], second[i]
    return [[(a, 0), (b, half)] for a, b in zip(first, second)]


def outward(blocks):
    half = blocks // 2
    moves = [[(0, 1), (half, 2)]]
    moves += [[(half, b)] for b in range(3, blocks) if b != half]
    return moves


def local(kv_cache, queries, new_latent, page_counts, page_tails, page_slots):
    _, pages, width, depth = kv_cache.shape
    _, batch, heads, _ = queries.shape
    rows = batch * heads
    blocks, members = lax.axis_size("ctx_block"), lax.axis_size("ctx_place")
    kv = jnp.swapaxes(kv_cache[0], 1, 2)
    q = queries[0].reshape(rows, depth)
    new = new_latent[0]
    block = lax.axis_index("ctx_block").reshape(1)
    place = lax.axis_index(CTX).reshape(1)
    vmem = pl.BlockSpec(memory_space=pltpu.VMEM)
    smem = pl.BlockSpec(memory_space=pltpu.SMEM)
    hbm = pl.BlockSpec(memory_space=pl.ANY)
    f32 = jnp.float32
    size = rows // members
    packed = packed_rows(size)
    partials = pl.pallas_call(
        partial_kernel,
        out_shape=pltpu.VMEM((members, packed, LANES), f32),
        in_specs=[smem, smem, smem, vmem, vmem, vmem, hbm],
        out_specs=vmem,
        scratch_shapes=[
            pltpu.VMEM((pages, depth, width), kv.dtype),
            pltpu.VMEM((rows, pages * width), f32),
            pltpu.VMEM((batch, pages, width), f32),
            pltpu.SemaphoreType.DMA((pages // CHUNK,)),
        ],
        name="partials",
    )(place, page_counts, page_tails, page_slots, q, new, kv)
    partials = lax.all_to_all(partials, "ctx_place", 0, 0, tiled=True)
    mine = pl.pallas_call(
        merge_kernel,
        out_shape=pltpu.VMEM((packed, LANES), f32),
        in_specs=[vmem],
        out_specs=vmem,
        name="merge",
    )(near(partials))

    def sent(x, moves):
        return lax.ppermute(x, CTX, [(s * members + j, t * members + j) for s, t in moves for j in range(members)])

    gathered = [sent(mine, moves) for moves in reversed(inward(blocks))]
    share = pl.pallas_call(
        close_kernel,
        out_shape=pltpu.VMEM((packed - 8, LANES), f32),
        in_specs=[vmem] * blocks,
        out_specs=vmem,
        name="close",
    )(near(mine), *map(near, gathered))
    spread = [sent(share, moves) for moves in reversed(outward(blocks))]
    shares = pl.pallas_call(
        choose_kernel,
        out_shape=pltpu.VMEM((members, *share.shape), f32),
        in_specs=[smem] + [vmem] * (1 + len(spread)),
        out_specs=vmem,
        name="choose",
    )(block, near(share), *map(near, spread))
    shares = lax.all_to_all(shares, "ctx_place", 0, 0, tiled=True)
    out = pl.pallas_call(
        unpack_kernel,
        out_shape=jax.ShapeDtypeStruct((rows, LATENT), jnp.bfloat16),
        in_specs=[vmem],
        out_specs=vmem,
        name="unpack",
    )(near(shares))
    return out.reshape(1, batch, heads, LATENT)


def solution(mesh):
    groups, ctx, head, rep = (mesh.shape[a] for a in ("groups", "ctx", "head", "rep"))
    devices = mesh.devices.reshape(groups, ctx // BLOCK, BLOCK, head, rep)
    split = Mesh(devices, ("groups", *CTX, "head", "rep"))
    in_specs = (
        P(("groups", "rep"), CTX, None, None),
        P(("groups", "rep"), None, "head", None),
        P(("groups", "rep"), None, None),
        P(("groups", "rep"), None),
        P(("groups", "rep"), None),
        P(("groups", "rep"), None),
    )
    out_specs = P(("groups", "rep"), None, "head", None)
    return jax.shard_map(local, mesh=split, in_specs=in_specs, out_specs=out_specs, check_vma=False)
```

```python
import jax
import jax.numpy as jnp
from jax import lax
from jax.experimental import pallas as pl
from jax.experimental.pallas import tpu as pltpu
from jax.sharding import Mesh, PartitionSpec as P

LATENT = 512
CHUNK = 4
BLOCK = 4


score_scale = 192.0 ** (-0.5)
neg_large = -1e30
CTX = ("ctx_block", "ctx_place")


def as_row(col):
    shape = (col.shape[0], col.shape[0])
    diagonal = lax.broadcasted_iota(jnp.int32, shape, 0) == lax.broadcasted_iota(jnp.int32, shape, 1)
    return jnp.sum(jnp.where(diagonal, col, 0.0), axis=0, keepdims=True)


def tail_tile(top, total):
    at = lax.broadcasted_iota(jnp.int32, (8, top.shape[1]), 0)
    return jnp.where(at == 0, top, jnp.where(at == 1, total, 0.0))


def minor_dot(a, b):
    return lax.dot_general(a, b, (((1,), (1,)), ((), ())), preferred_element_type=jnp.float32)


def fetch(kv_ref, kv_buf, sems):
    copies = []
    for i in range(kv_buf.shape[0] // CHUNK):
        part = pl.ds(i * CHUNK, CHUNK)
        copy = pltpu.make_async_copy(kv_ref.at[part], kv_buf.at[part], sems.at[i])
        copy.start()
        copies.append(copy)
    return copies


def partial_kernel(place_ref, counts_ref, tails_ref, slots_ref, q_ref, new_ref, kv_ref, out_ref, kv_buf, s_buf, bias_ref, sems):
    copies = fetch(kv_ref, kv_buf, sems)
    pages, _, width = kv_buf.shape
    rows = q_ref.shape[0]
    batch = new_ref.shape[0]
    heads = rows // batch
    slots = slots_ref[...]
    slot_ids = place_ref[0] * pages + lax.broadcasted_iota(jnp.int32, (pages, slots.shape[1]), 0)
    ranks_at = lax.broadcasted_iota(jnp.int32, (pages, slots.shape[1]), 1)
    rank = jnp.sum(jnp.where(slots == slot_ids, ranks_at, 0), axis=1, keepdims=True)
    token = lax.broadcasted_iota(jnp.int32, (pages, width), 1)
    start = jnp.int32(0)
    for b in range(batch):
        count = counts_ref[0, b]
        end = start + count
        length = (count - 1) * width + tails_ref[0, b]
        inside = (rank >= start) & (rank < end)
        limit = jnp.where(inside, length - (rank - start) * width, 0)
        bias_ref[b] = jnp.where(token < limit, 0.0, neg_large)
        start = end
    q = q_ref[...]
    new = new_ref[...]
    row_of = lax.broadcasted_iota(jnp.int32, (rows, batch), 0) // heads
    mine = row_of == lax.broadcasted_iota(jnp.int32, (rows, batch), 1)
    own = jnp.sum(jnp.where(mine, minor_dot(q, new), 0.0), axis=1, keepdims=True) * score_scale
    best = [jnp.full((heads, width), neg_large, jnp.float32) for _ in range(batch)]
    for i, copy in enumerate(copies):
        copy.wait()
        keys = jnp.concatenate([kv_buf[i * CHUNK + j] for j in range(CHUNK)], axis=1)
        scores = jnp.dot(q, keys, preferred_element_type=jnp.float32) * score_scale
        for j in range(CHUNK):
            p = i * CHUNK + j
            for b in range(batch):
                tile = scores[b * heads : (b + 1) * heads, j * width : (j + 1) * width] + bias_ref[b, p : p + 1, :]
                best[b] = jnp.maximum(best[b], tile)
                s_buf[b * heads : (b + 1) * heads, p * width : (p + 1) * width] = tile
    top = jnp.maximum(jnp.max(jnp.concatenate(best, axis=0), axis=1, keepdims=True), own)
    span = CHUNK * width
    ones = jnp.ones((8, span), jnp.bfloat16)
    total = jnp.zeros((8, rows), jnp.float32)
    acc = jnp.zeros((LATENT, rows), jnp.float32)
    for i in range(len(copies)):
        weights = jnp.exp(s_buf[:, i * span : (i + 1) * span] - top).astype(jnp.bfloat16)
        values = jnp.concatenate([kv_buf[i * CHUNK + j, :LATENT, :] for j in range(CHUNK)], axis=1)
        acc = acc + minor_dot(values, weights)
        total = total + minor_dot(ones, weights)
    top_row = as_row(top)
    own_weight = jnp.where(place_ref[0] == 0, jnp.exp(as_row(own) - top_row), 0.0)
    members = out_ref.shape[0]
    size = LATENT // members
    tail = tail_tile(top_row, total[:1] + own_weight)
    for j in range(members):
        out_ref[j, :size, :] = acc[j * size : (j + 1) * size]
        out_ref[j, size:, :] = tail

    @pl.when(place_ref[0] == 0)
    def _():
        shape = (batch, rows)
        at = lax.broadcasted_iota(jnp.int32, shape, 0) == lax.broadcasted_iota(jnp.int32, shape, 1) // heads
        spread = jnp.where(at, own_weight, 0.0)
        row = new_ref[:, :LATENT].astype(jnp.float32)
        added = lax.dot_general(
            row, spread, (((0,), (0,)), ((), ())), precision=lax.Precision.HIGHEST, preferred_element_type=jnp.float32
        )
        for j in range(members):
            out_ref[j, :size, :] += added[j * size : (j + 1) * size]


def merged(pieces):
    size = pieces[0].shape[0] - 8
    tops = [piece[size : size + 1, :] for piece in pieces]
    top = tops[0]
    for other in tops[1:]:
        top = jnp.maximum(top, other)
    factors = [jnp.exp(t - top) for t in tops]
    total = sum(f * piece[size + 1 : size + 2, :] for f, piece in zip(factors, pieces))
    acc = sum(f * piece[:size, :] for f, piece in zip(factors, pieces))
    return top, total, acc


def merge_kernel(in_ref, out_ref):
    top, total, acc = merged([in_ref.at[i] for i in range(in_ref.shape[0])])
    size = acc.shape[0]
    out_ref[:size, :] = acc
    out_ref[size:, :] = tail_tile(top, total)


def close_kernel(*refs):
    _, total, acc = merged(refs[:-1])
    refs[-1][...] = acc / total


def choose_kernel(block_ref, own_ref, *refs):
    others, out_ref = refs[:-1], refs[-1]
    arrived = others[0][...]
    for other in others[1:]:
        arrived = arrived + other[...]
    blocks = lax.axis_size(CTX[0])
    closes = (block_ref[0] == 0) | (block_ref[0] == blocks // 2 - 1)
    share = jnp.where(closes, own_ref[...], arrived)
    for j in range(out_ref.shape[0]):
        out_ref[j] = share


def unpack_kernel(in_ref, out_ref):
    members, size, _ = in_ref.shape
    for j in range(members):
        out_ref[:, j * size : (j + 1) * size] = in_ref[j].T.astype(out_ref.dtype)


def near(x):
    return pltpu.with_memory_space_constraint(x, pltpu.VMEM)


def inward(blocks):
    second = blocks // 2 - 1
    late = list(range(blocks - 1, second, -1))
    early = list(range(second, 0, -1))
    moves = [[(late[0], 0), (late[1], second)], [(late[-1], 0), (late[0], second)]]
    moves += [[(late[1], 0), (late[2], second)], [(early[0], 0), (late[3], second)]]
    moves += [[(late[2], 0), (early[1], second)]]
    moves += [[(early[i], 0), (early[i] - 1, second)] for i in range(1, len(early))]
    return moves


def outward(blocks):
    second = blocks // 2 - 1
    moves = [[(0, 1), (second, second - 1)]]
    moves += [[(second, b)] for b in range(second + 1, blocks)]
    return moves


def local(kv_cache, queries, new_latent, page_counts, page_tails, page_slots):
    _, pages, width, depth = kv_cache.shape
    _, batch, heads, _ = queries.shape
    rows = batch * heads
    blocks, members = lax.axis_size("ctx_block"), lax.axis_size("ctx_place")
    kv = jnp.swapaxes(kv_cache[0], 1, 2)
    q = queries[0].reshape(rows, depth)
    new = new_latent[0]
    block = lax.axis_index("ctx_block").reshape(1)
    place = lax.axis_index(CTX).reshape(1)
    vmem = pl.BlockSpec(memory_space=pltpu.VMEM)
    smem = pl.BlockSpec(memory_space=pltpu.SMEM)
    hbm = pl.BlockSpec(memory_space=pl.ANY)
    f32 = jnp.float32
    packed = LATENT // members + 8
    partials = pl.pallas_call(
        partial_kernel,
        out_shape=pltpu.VMEM((members, packed, rows), f32),
        in_specs=[smem, smem, smem, vmem, vmem, vmem, hbm],
        out_specs=vmem,
        scratch_shapes=[
            pltpu.VMEM((pages, depth, width), kv.dtype),
            pltpu.VMEM((rows, pages * width), f32),
            pltpu.VMEM((batch, pages, width), f32),
            pltpu.SemaphoreType.DMA((pages // CHUNK,)),
        ],
        name="partials",
    )(place, page_counts, page_tails, page_slots, q, new, kv)
    partials = lax.all_to_all(partials, "ctx_place", 0, 0, tiled=True)
    mine = pl.pallas_call(
        merge_kernel,
        out_shape=pltpu.VMEM((packed, rows), f32),
        in_specs=[vmem],
        out_specs=vmem,
        name="merge",
    )(near(partials))

    def sent(x, moves):
        return lax.ppermute(x, CTX, [(s * members + j, t * members + j) for s, t in moves for j in range(members)])

    gathered = [sent(mine, moves) for moves in reversed(inward(blocks))]
    share = pl.pallas_call(
        close_kernel,
        out_shape=pltpu.VMEM((packed - 8, rows), f32),
        in_specs=[vmem] * blocks,
        out_specs=vmem,
        name="close",
    )(near(mine), *map(near, gathered))
    spread = [sent(share, moves) for moves in reversed(outward(blocks))]
    shares = pl.pallas_call(
        choose_kernel,
        out_shape=pltpu.VMEM((members, *share.shape), f32),
        in_specs=[smem] + [vmem] * (1 + len(spread)),
        out_specs=vmem,
        name="choose",
    )(block, near(share), *map(near, spread))
    shares = lax.all_to_all(shares, "ctx_place", 0, 0, tiled=True)
    out = pl.pallas_call(
        unpack_kernel,
        out_shape=jax.ShapeDtypeStruct((rows, LATENT), jnp.bfloat16),
        in_specs=[vmem],
        out_specs=vmem,
        name="unpack",
    )(near(shares))
    return out.reshape(1, batch, heads, LATENT)


def solution(mesh):
    groups, ctx, head, rep = (mesh.shape[a] for a in ("groups", "ctx", "head", "rep"))
    devices = mesh.devices.reshape(groups, ctx // BLOCK, BLOCK, head, rep)
    split = Mesh(devices, ("groups", *CTX, "head", "rep"))
    in_specs = (
        P(("groups", "rep"), CTX, None, None),
        P(("groups", "rep"), None, "head", None),
        P(("groups", "rep"), None, None),
        P(("groups", "rep"), None),
        P(("groups", "rep"), None),
        P(("groups", "rep"), None),
    )
    out_specs = P(("groups", "rep"), None, "head", None)
    return jax.shard_map(local, mesh=split, in_specs=in_specs, out_specs=out_specs, check_vma=False)
```

```python
import jax
import jax.numpy as jnp
from jax import lax
from jax.experimental import pallas as pl
from jax.experimental.pallas import tpu as pltpu
from jax.sharding import Mesh, PartitionSpec as P

LATENT = 512
CHUNK = 4
BLOCK = 4


score_scale = 192.0 ** (-0.5)
neg_large = -1e30
CTX = ("ctx_block", "ctx_place")


def as_row(col):
    shape = (col.shape[0], col.shape[0])
    diagonal = lax.broadcasted_iota(jnp.int32, shape, 0) == lax.broadcasted_iota(jnp.int32, shape, 1)
    return jnp.sum(jnp.where(diagonal, col, 0.0), axis=0, keepdims=True)


def tail_tile(top, total):
    at = lax.broadcasted_iota(jnp.int32, (8, top.shape[1]), 0)
    return jnp.where(at == 0, top, jnp.where(at == 1, total, 0.0))


def minor_dot(a, b):
    return lax.dot_general(a, b, (((1,), (1,)), ((), ())), preferred_element_type=jnp.float32)


def partial_kernel(place_ref, *refs):
    sources, out_ref, (counts_ref, tails_ref, slots_ref, q_ref, new_ref, kv_buf) = refs[:6], refs[6], refs[7:13]
    s_buf, bias_ref, small_sems, sems = refs[13:]
    pages, _, width = kv_buf.shape
    targets = (counts_ref, tails_ref, slots_ref, q_ref, new_ref)
    small = [pltpu.make_async_copy(s, t, small_sems.at[i]) for i, (s, t) in enumerate(zip(sources, targets))]
    parts = [pl.ds(i * CHUNK, CHUNK) for i in range(pages // CHUNK)]
    copies = [pltpu.make_async_copy(sources[5].at[p], kv_buf.at[p], sems.at[i]) for i, p in enumerate(parts)]
    for copy in small + copies:
        copy.start()
    for copy in small:
        copy.wait()
    rows = q_ref.shape[0]
    batch = new_ref.shape[0]
    heads = rows // batch
    slots = slots_ref[...]
    slot_ids = place_ref[0] * pages + lax.broadcasted_iota(jnp.int32, (pages, slots.shape[1]), 0)
    ranks_at = lax.broadcasted_iota(jnp.int32, (pages, slots.shape[1]), 1)
    rank = jnp.sum(jnp.where(slots == slot_ids, ranks_at, 0), axis=1, keepdims=True)
    token = lax.broadcasted_iota(jnp.int32, (pages, width), 1)
    start = jnp.int32(0)
    for b in range(batch):
        count = counts_ref[0, b]
        end = start + count
        length = (count - 1) * width + tails_ref[0, b]
        inside = (rank >= start) & (rank < end)
        limit = jnp.where(inside, length - (rank - start) * width, 0)
        bias_ref[b] = jnp.where(token < limit, 0.0, neg_large)
        start = end
    q = q_ref[...]
    new = new_ref[...]
    row_of = lax.broadcasted_iota(jnp.int32, (rows, batch), 0) // heads
    mine = row_of == lax.broadcasted_iota(jnp.int32, (rows, batch), 1)
    own = jnp.sum(jnp.where(mine, minor_dot(q, new), 0.0), axis=1, keepdims=True) * score_scale
    best = [jnp.full((heads, width), neg_large, jnp.float32) for _ in range(batch)]
    for i, copy in enumerate(copies):
        copy.wait()
        keys = jnp.concatenate([kv_buf[i * CHUNK + j] for j in range(CHUNK)], axis=1)
        scores = jnp.dot(q, keys, preferred_element_type=jnp.float32) * score_scale
        for j in range(CHUNK):
            p = i * CHUNK + j
            for b in range(batch):
                tile = scores[b * heads : (b + 1) * heads, j * width : (j + 1) * width] + bias_ref[b, p : p + 1, :]
                best[b] = jnp.maximum(best[b], tile)
                s_buf[b * heads : (b + 1) * heads, p * width : (p + 1) * width] = tile
    top = jnp.maximum(jnp.max(jnp.concatenate(best, axis=0), axis=1, keepdims=True), own)
    span = CHUNK * width
    ones = jnp.ones((8, span), jnp.bfloat16)
    total = jnp.zeros((8, rows), jnp.float32)
    acc = jnp.zeros((LATENT, rows), jnp.float32)
    for i in range(len(copies)):
        weights = jnp.exp(s_buf[:, i * span : (i + 1) * span] - top).astype(jnp.bfloat16)
        values = jnp.concatenate([kv_buf[i * CHUNK + j, :LATENT, :] for j in range(CHUNK)], axis=1)
        acc = acc + minor_dot(values, weights)
        total = total + minor_dot(ones, weights)
    top_row = as_row(top)
    own_weight = jnp.where(place_ref[0] == 0, jnp.exp(as_row(own) - top_row), 0.0)
    members = out_ref.shape[0]
    size = LATENT // members
    tail = tail_tile(top_row, total[:1] + own_weight)
    for j in range(members):
        out_ref[j, :size, :] = acc[j * size : (j + 1) * size]
        out_ref[j, size:, :] = tail

    @pl.when(place_ref[0] == 0)
    def _():
        shape = (batch, rows)
        at = lax.broadcasted_iota(jnp.int32, shape, 0) == lax.broadcasted_iota(jnp.int32, shape, 1) // heads
        spread = jnp.where(at, own_weight, 0.0)
        row = new_ref[:, :LATENT].astype(jnp.float32)
        added = lax.dot_general(
            row, spread, (((0,), (0,)), ((), ())), precision=lax.Precision.HIGHEST, preferred_element_type=jnp.float32
        )
        for j in range(members):
            out_ref[j, :size, :] += added[j * size : (j + 1) * size]


def merged(pieces):
    size = pieces[0].shape[0] - 8
    sums = [piece[size + 1 : size + 2, :] for piece in pieces]
    tops = [jnp.where(t > 0.0, piece[size : size + 1, :], neg_large) for t, piece in zip(sums, pieces)]
    top = tops[0]
    for other in tops[1:]:
        top = jnp.maximum(top, other)
    factors = [jnp.exp(t - top) for t in tops]
    total = sum(f * t for f, t in zip(factors, sums))
    acc = sum(f * piece[:size, :] for f, piece in zip(factors, pieces))
    return top, total, acc


def write_packed(out_ref, top, total, acc):
    size = acc.shape[0]
    out_ref[:size, :] = acc
    out_ref[size:, :] = tail_tile(top, total)


def merge_kernel(in_ref, out_ref):
    write_packed(out_ref, *merged([in_ref.at[i] for i in range(in_ref.shape[0])]))


def join_kernel(one_ref, other_ref, out_ref):
    write_packed(out_ref, *merged([one_ref, other_ref]))


def close_kernel(*refs):
    _, total, acc = merged(refs[:-1])
    refs[-1][...] = acc / total


def choose_kernel(block_ref, own_ref, *refs):
    others, out_ref = refs[:-1], refs[-1]
    arrived = others[0][...]
    for other in others[1:]:
        arrived = arrived + other[...]
    blocks = lax.axis_size(CTX[0])
    closes = (block_ref[0] == 0) | (block_ref[0] == blocks // 2)
    share = jnp.where(closes, own_ref[...], arrived)
    for j in range(out_ref.shape[0]):
        out_ref[j] = share


def unpack_kernel(in_ref, out_ref):
    members, size, _ = in_ref.shape
    for j in range(members):
        out_ref[:, j * size : (j + 1) * size] = in_ref[j].T.astype(out_ref.dtype)


def near(x):
    return pltpu.with_memory_space_constraint(x, pltpu.VMEM)


def inward(blocks):
    second = blocks // 2
    late = list(range(blocks - 1, second, -1))
    moves = [[(late[0], 0)]]
    moves += [[(b, 0), (b + 1, second)] for b in late[1:] + [second]]
    moves += [[(3, 0)], [(1, 0), (3, second)], [(2, 0), (1, second)]]
    return moves


def outward(blocks):
    second = blocks // 2
    moves = [[(0, 1), (second, 2)], [(second, 3)]]
    moves += [[(second, b)] for b in range(second + 1, blocks)]
    return moves


def local(kv_cache, queries, new_latent, page_counts, page_tails, page_slots):
    _, pages, width, depth = kv_cache.shape
    _, batch, heads, _ = queries.shape
    rows = batch * heads
    blocks, members = lax.axis_size("ctx_block"), lax.axis_size("ctx_place")
    kv = jnp.swapaxes(kv_cache[0], 1, 2)
    q = queries[0].reshape(rows, depth)
    new = new_latent[0]
    block = lax.axis_index("ctx_block").reshape(1)
    place = lax.axis_index(CTX).reshape(1)
    vmem = pl.BlockSpec(memory_space=pltpu.VMEM)
    smem = pl.BlockSpec(memory_space=pltpu.SMEM)
    hbm = pl.BlockSpec(memory_space=pl.ANY)
    f32 = jnp.float32
    packed = LATENT // members + 8
    partials = pl.pallas_call(
        partial_kernel,
        out_shape=pltpu.VMEM((members, packed, rows), f32),
        in_specs=[smem] + [hbm] * 6,
        out_specs=vmem,
        scratch_shapes=[
            pltpu.SMEM(page_counts.shape, page_counts.dtype),
            pltpu.SMEM(page_tails.shape, page_tails.dtype),
            pltpu.VMEM(page_slots.shape, page_slots.dtype),
            pltpu.VMEM(q.shape, q.dtype),
            pltpu.VMEM(new.shape, new.dtype),
            pltpu.VMEM(kv.shape, kv.dtype),
            pltpu.VMEM((rows, pages * width), f32),
            pltpu.VMEM((batch, pages, width), f32),
            pltpu.SemaphoreType.DMA((5,)),
            pltpu.SemaphoreType.DMA((pages // CHUNK,)),
        ],
        name="partials",
    )(place, page_counts, page_tails, page_slots, q, new, kv)
    partials = lax.all_to_all(partials, "ctx_place", 0, 0, tiled=True)
    mine = pl.pallas_call(
        merge_kernel,
        out_shape=pltpu.VMEM((packed, rows), f32),
        in_specs=[vmem],
        out_specs=vmem,
        name="merge",
    )(near(partials))

    def sent(x, moves):
        return lax.ppermute(x, CTX, [(s * members + j, t * members + j) for s, t in moves for j in range(members)])

    moves = inward(blocks)
    gathered = [sent(mine, m) for m in reversed(moves[3:])]
    first_part = sent(mine, [(0, 2)])
    gathered += [sent(mine, m) for m in reversed(moves[:3])]
    joined = pl.pallas_call(
        join_kernel,
        out_shape=pltpu.VMEM((packed, rows), f32),
        in_specs=[vmem] * 2,
        out_specs=vmem,
        name="join",
    )(near(mine), near(first_part))
    gathered.append(sent(joined, [(2, blocks // 2)]))
    share = pl.pallas_call(
        close_kernel,
        out_shape=pltpu.VMEM((packed - 8, rows), f32),
        in_specs=[vmem] * (1 + len(gathered)),
        out_specs=vmem,
        name="close",
    )(near(mine), *map(near, gathered))
    spread = [sent(share, moves) for moves in reversed(outward(blocks))]
    shares = pl.pallas_call(
        choose_kernel,
        out_shape=pltpu.VMEM((members, *share.shape), f32),
        in_specs=[smem] + [vmem] * (1 + len(spread)),
        out_specs=vmem,
        name="choose",
    )(block, near(share), *map(near, spread))
    shares = lax.all_to_all(shares, "ctx_place", 0, 0, tiled=True)
    out = pl.pallas_call(
        unpack_kernel,
        out_shape=jax.ShapeDtypeStruct((rows, LATENT), jnp.bfloat16),
        in_specs=[vmem],
        out_specs=vmem,
        name="unpack",
    )(near(shares))
    return out.reshape(1, batch, heads, LATENT)


def solution(mesh):
    groups, ctx, head, rep = (mesh.shape[a] for a in ("groups", "ctx", "head", "rep"))
    devices = mesh.devices.reshape(groups, ctx // BLOCK, BLOCK, head, rep)
    split = Mesh(devices, ("groups", *CTX, "head", "rep"))
    in_specs = (
        P(("groups", "rep"), CTX, None, None),
        P(("groups", "rep"), None, "head", None),
        P(("groups", "rep"), None, None),
        P(("groups", "rep"), None),
        P(("groups", "rep"), None),
        P(("groups", "rep"), None),
    )
    out_specs = P(("groups", "rep"), None, "head", None)
    return jax.shard_map(local, mesh=split, in_specs=in_specs, out_specs=out_specs, check_vma=False)
```
